32 devices in a mesh: aa: 2 (over core), ba: 16 (over z, y, x).
Axes of the slice: x: 2, y: 2, z: 4, core: 2. Of those that a mesh axis runs over, the one named last changes fastest.
Arguments:
- queries: bfloat16 [2, 16, 192, 1024], P('aa', 'ba'), may hold values from -6 to 6
- key_rows: bfloat16 [2, 16, 192, 1024], P('aa', 'ba'), may hold values from -6 to 6
- value_rows: bfloat16 [2, 16, 192, 1024], P('aa', 'ba'), may hold values from -6 to 6
- out_proj: bfloat16 [2, 1024, 1024], P('aa', 'ba'), may hold values from -0.1875 to 0.1875
- scale_ids: int32 [16, 192], P('ba'), may hold values from 0 to 7, never falling along the last dimension, each value on 1 to 64 neighbouring positions
- residual_in: bfloat16 [16, 192, 1024], P('ba'), may hold values from -4 to 4
- cotangent: bfloat16 [16, 192, 1024], P('ba'), may hold values from -6 to 6
Outputs:
- residual_out: bfloat16 [2, 16, 192, 1024], P('aa', 'ba')
- grad_query: bfloat16 [2, 16, 192, 1024], P('aa', 'ba')
- grad_key: bfloat16 [2, 16, 192, 1024], P('aa', 'ba')
- grad_value: bfloat16 [2, 16, 192, 1024], P('aa', 'ba')
- grad_proj: float32 [2, 1024, 1024], P('aa', 'ba')
The draws below stay inside these ranges and needn't reach their ends.
Inputs may be any that keep to these rules, and one draw needn't show every extreme that they name: `scale_ids`: for each image the scale ids never fall along the tokens; every scale from 0 to 7 is present, with 1 to 64 tokens.
All inputs are finite; a program needn't handle non-finite values.
Results may differ from the reference program's by a relative error of at most 0.0086.
Values may be sent and summed in bfloat16 or wider, within the bound.
No kernel may reach another device: no remote copies, remote signals or barrier semaphores. Data moves between devices by JAX's collectives and lax.ppermute only.
A program may use at most 64 MiB of HBM per device.

```python
import math
import jax
import jax.numpy as jnp
import numpy as np
from jax import lax

HEADS = 16
HD = 64
RES = 1024
SEQ = 192
SCALES = 8
MOST = 64
INNER = 1024
IMAGES = 16
SECTIONS = 2


def query_key_pair(key):
    seeded = jax.random.fold_in(key, 9173)
    full_shape = (SECTIONS, IMAGES, SEQ, HEADS * HD)
    queries = jnp.clip(jax.random.normal(jax.random.fold_in(seeded, 5), full_shape, jnp.float32), -5.0, 5.0)
    key_rows = jnp.clip(jax.random.normal(jax.random.fold_in(seeded, 6), full_shape, jnp.float32), -5.0, 5.0)
    return (queries, key_rows)


def draw_queries(key, part):
    return query_key_pair(key)[0].astype(jnp.bfloat16)


def draw_key_rows(key, part):
    return query_key_pair(key)[1].astype(jnp.bfloat16)


def spiked(entries, key, source, target, parts, factor):
    def block_of(dim):
        return (jnp.arange(entries.shape[dim]) // (entries.shape[dim] // parts)).reshape((-1,) + (1,) * (entries.ndim - 1 - dim))

    near = jax.random.permutation(key, parts)[block_of(target)]
    far = (block_of(target) + parts // 2) % parts
    return jnp.where((block_of(source) == near) | (block_of(source) == far), factor * entries, entries)


def steps_of(rng, dims, split, smallest, high):
    loudness = 1.0
    for position, parts in split:
        draws = jax.random.uniform(jax.random.fold_in(jax.random.fold_in(rng, 6), position), (parts,), jnp.float32, smallest / len(split), high / len(split))
        loudness = loudness * jnp.repeat(jnp.exp(draws), dims[position] // parts).reshape((-1,) + (1,) * (len(dims) - 1 - position))
    return loudness


def length_profile(amount, total, most, lean):
    weights = [(1 << 20) // math.isqrt(rank ** lean) + 1 for rank in range(2, amount + 1)]
    rest, holding = total - most - (amount - 1), [1] * (amount - 1)
    while rest > 0:
        free = [i for i in range(amount - 1) if holding[i] < most]
        whole, budget = sum([weights[i] for i in free]), rest
        for i in free:
            more = min(most - holding[i], max(1, budget * weights[i] // whole), rest)
            holding[i] = holding[i] + more
            rest = rest - more
    return np.array([most] + holding)


def uneven(stream_key, count, total, reach, lean):
    if count == 2:
        one = jax.random.randint(stream_key, (), max(1, total - reach), min(reach, total - 1) + 1)
        return jnp.stack([one, total - one])
    tallies = jnp.asarray(length_profile(count, total, reach, lean), jnp.int32)
    couples = (count - 1) // 2
    donor, receiver = tallies[1:1 + 2 * couples:2], tallies[2:2 + 2 * couples:2]
    margin = jnp.minimum(donor - 1, reach - receiver)
    moved = jax.random.randint(jax.random.fold_in(stream_key, 1), (couples,), 0, 1 << 20) % (margin + 1)
    tallies = tallies.at[1:1 + 2 * couples:2].set(donor - moved).at[2:2 + 2 * couples:2].set(receiver + moved)
    return tallies[jax.random.permutation(jax.random.fold_in(stream_key, 2), count)]


def gaussian(key, extent, scale, limit, pieces=(), held_as=jnp.bfloat16):
    entries = jax.random.normal(key, extent, jnp.float32) * scale
    if len(pieces) > 0:
        entries = steps_of(key, extent, pieces, -0.22, 0.18) * entries
    return jnp.clip(entries, min=-limit, max=limit).astype(held_as)


def bell_draw_with(key, shape, scale, reach, pieces, heavy, held_as=jnp.bfloat16):
    array = scale * jax.random.normal(key, shape, jnp.float32)
    if pieces:
        array = array * steps_of(key, shape, pieces, -0.22, 0.18)
    return jnp.clip(spiked(array, jax.random.fold_in(key, 3), *heavy), -reach, reach).astype(held_as)


def setup_inputs(seed: int = 0) -> dict:
    keys = jax.random.split(jax.random.key(seed), 8)
    queries = draw_queries(jax.random.fold_in(keys[7], 71), 0)
    key_rows = draw_key_rows(jax.random.fold_in(keys[7], 71), 0)
    value_rows = bell_draw_with(keys[2], (SECTIONS, IMAGES, SEQ, INNER), 1.0, 6.0, ((0, 2), (1, 16)), (1, 3, 16, 2.0))
    out_proj = gaussian(keys[3], (SECTIONS, INNER, RES), INNER ** -0.5, 0.1875, ((0, 2), (1, 16)))
    scale_ids = jax.vmap(lambda own: jnp.searchsorted(jnp.cumsum(uneven(own, SCALES, SEQ, MOST, 2)), jnp.arange(SEQ), side="right"))(jax.random.split(keys[4], IMAGES)).reshape((IMAGES, SEQ)).astype(jnp.int32)
    residual_in = gaussian(keys[5], (IMAGES, SEQ, RES), 0.3, 4.0, ((0, 16),))
    cotangent = gaussian(keys[6], (IMAGES, SEQ, RES), 1.0, 6.0, ((0, 16),))
    return dict(queries=queries, key_rows=key_rows, value_rows=value_rows, out_proj=out_proj, scale_ids=scale_ids, residual_in=residual_in, cotangent=cotangent)


def round_low(values):
    return lax.optimization_barrier(values.astype(jnp.bfloat16)).astype(jnp.float32)


def reference(queries, key_rows, value_rows, out_proj, scale_ids, residual_in, cotangent):
    images = scale_ids.shape[0]
    length = scale_ids.shape[1]
    score_scale = HD ** -0.5
    visible = scale_ids[:, None, :] <= scale_ids[:, :, None]
    cot_rows = cotangent.reshape(images * length, RES)

    def section_pass(running, operands):
        q_all, k_all, v_all, w_out = operands
        q_heads = q_all.reshape(images, length, HEADS, HD).astype(jnp.float32)
        k_heads = k_all.reshape(images, length, HEADS, HD).astype(jnp.float32)
        v_heads = v_all.reshape(images, length, HEADS, HD).astype(jnp.float32)
        scores = jnp.einsum("bihd,bjhd->bhij", q_heads, k_heads) * score_scale
        scores = jnp.where(visible[:, None], scores, -jnp.inf)
        row_max = jnp.max(scores, axis=-1, keepdims=True)
        lifted = jnp.exp(scores - row_max)
        attn_probs = lifted / jnp.sum(lifted, axis=-1, keepdims=True)
        probs_low = round_low(attn_probs)
        attended = jnp.einsum("bhij,bjhd->bihd", probs_low, v_heads)
        attended = attended.astype(jnp.bfloat16).reshape(images * length, INNER)
        branch = jnp.dot(attended, w_out, preferred_element_type=jnp.float32)
        running_next = running + branch.reshape(images, length, RES)
        d_attn = round_low(jnp.dot(cot_rows, w_out.T, preferred_element_type=jnp.float32))
        grad_proj = lax.dot_general(attended, cot_rows, (((0,), (0,)), ((), ())), preferred_element_type=jnp.float32) / IMAGES
        d_heads = d_attn.reshape(images, length, HEADS, HD)
        grad_value = jnp.einsum("bhij,bihd->bjhd", probs_low, d_heads)
        d_probs = jnp.einsum("bihd,bjhd->bhij", d_heads, v_heads)
        row_delta = jnp.sum(attn_probs * d_probs, axis=-1, keepdims=True)
        d_scores = round_low(attn_probs * (d_probs - row_delta) * score_scale)
        grad_query = jnp.einsum("bhij,bjhd->bihd", d_scores, k_heads)
        grad_key = jnp.einsum("bhij,bihd->bjhd", d_scores, q_heads)
        outputs = (
            running_next.astype(jnp.bfloat16),
            grad_query.reshape(images, length, INNER).astype(jnp.bfloat16),
            grad_key.reshape(images, length, INNER).astype(jnp.bfloat16),
            grad_value.reshape(images, length, INNER).astype(jnp.bfloat16),
            grad_proj,
        )
        return running_next, outputs

    start_value = residual_in.astype(jnp.float32)
    final_value, stacked = lax.scan(section_pass, start_value, (queries, key_rows, value_rows, out_proj))
    return stacked[0], stacked[1], stacked[2], stacked[3], stacked[4]
```

```python
import functools

import jax
import jax.numpy as jnp
from jax import lax
from jax.experimental import pallas as pl
from jax.experimental.pallas import tpu as pltpu
from jax.sharding import PartitionSpec as P

HD = 64
LANES = 128


VMEM = pl.BlockSpec(memory_space=pltpu.VMEM)
SMEM = pl.BlockSpec(memory_space=pltpu.SMEM)
NT = (((1,), (1,)), ((), ()))
TN = (((0,), (0,)), ((), ()))
PARAMS = pltpu.CompilerParams(vmem_limit_bytes=24 << 20)
F32 = jnp.float32
BF16 = jnp.bfloat16


def mul(a, b, dims):
    return lax.dot_general(a, b, dims, preferred_element_type=F32)


def nn(a, b):
    return jnp.dot(a, b, preferred_element_type=F32)


def tile(index):
    return pl.ds(pl.multiple_of(index * LANES, LANES), LANES)


def first_head(shape):
    return lax.broadcasted_iota(jnp.int32, shape, 1) < HD


def call(body, outs, flops, name, aliases=None, n_smem=1, n_vmem=0, scratch=()):
    return pl.pallas_call(
        body,
        out_shape=outs,
        in_specs=[SMEM] * n_smem + [VMEM] * n_vmem,
        out_specs=jax.tree.map(lambda _: VMEM, outs),
        scratch_shapes=list(scratch),
        compiler_params=PARAMS,
        cost_estimate=pl.CostEstimate(flops=flops, bytes_accessed=1 << 20, transcendentals=0),
        name=name,
    )


def forward_body(place, ids_row, ids_col, q_ref, k_ref, v_ref, attended, probs):
    own = place[0]
    length = q_ref.shape[0]
    visible = ids_col[...] <= ids_row[...]
    left = first_head((length, LANES))
    for pair in range(q_ref.shape[1] // LANES):
        cols = pl.ds(pair * LANES, LANES)
        q_pair = q_ref[:, cols] * (HD**-0.5)
        k_pair = k_ref[:, cols]
        v_pair = v_ref[:, cols]
        halves = []
        for half in range(2):
            k_head = jnp.where(left == (half == 0), k_pair, jnp.zeros_like(k_pair))
            scores = jnp.where(visible, mul(k_head, q_pair, NT), -jnp.inf)
            lifted = jnp.exp(scores - jnp.max(scores, axis=0, keepdims=True))
            low = (lifted * (1.0 / jnp.sum(lifted, axis=0, keepdims=True))).astype(BF16)
            probs[2 * pair + half] = low
            halves.append(mul(low, v_pair, TN))
        rows = jnp.where(left, halves[0], halves[1]).astype(BF16)
        attended[lax.rem(own + pair % 2, 2), :, pl.ds((pair // 2) * LANES, LANES)] = rows


def backward_body(shift, place, q_ref, k_ref, v_ref, d_ref, probs, *rest):
    targets = rest[-3:]
    kind = lax.rem(place[0] + shift, 2)
    length = q_ref.shape[0]
    left = first_head((length, LANES))
    for step in range(d_ref.shape[1] // LANES):
        for done, target in zip(rest[:-3], targets):
            cols = tile(2 * step + 1 - kind)
            target[:, cols] = done[:, cols]
        pair = 2 * step + kind
        cols = tile(pair)
        q_pair = q_ref[:, cols] * (HD**-0.5)
        k_pair = k_ref[:, cols] * (HD**-0.5)
        v_pair = v_ref[:, cols]
        d_pair = d_ref[:, pl.ds(step * LANES, LANES)]
        got = []
        for half in range(2):
            low = probs[2 * pair + half]
            wide = low.astype(F32)
            v_head = jnp.where(left == (half == 0), v_pair, jnp.zeros_like(v_pair))
            d_probs = mul(v_head, d_pair, NT)
            delta = jnp.sum(wide * d_probs, axis=0, keepdims=True)
            d_scores = (wide * (d_probs - delta)).astype(BF16)
            got.append((mul(d_scores, k_pair, TN), nn(d_scores, q_pair), nn(low, d_pair)))
        for target, one, two in zip(targets, got[0], got[1]):
            target[:, cols] = jnp.where(left, one, two).astype(BF16)


def product_body(first, weight, place, a_own, a_mate, c_own, c_mate, keep, send):
    upper, top = place[1], place[2]
    for step in range(keep.shape[0]):
        cols = tile(jnp.bitwise_xor(top, first + step))
        rows = mul(a_own[:, cols], c_own[...], TN) + mul(a_mate[:, cols], c_mate[...], TN)
        rows = rows * weight
        low, high = rows[:HD], rows[HD:]
        keep[step] = jnp.where(upper == 0, low, high)
        send[step] = jnp.where(upper == 0, high, low).astype(BF16)


def weights_body(place, near, near_x, far, far_x, a_mate, c_mate, send, w_out):
    upper, top = place[1], place[2]
    half = near.shape[0]
    for distance in range(2 * half):
        mine, other = (near, near_x) if distance < half else (far, far_x)
        base = jnp.bitwise_xor(top, distance) * LANES
        step = distance % half
        w_out[pl.ds(pl.multiple_of(base + upper * HD, HD), HD), :] = mine[step]
        w_out[pl.ds(pl.multiple_of(base + (1 - upper) * HD, HD), HD), :] = other[step]
    width = w_out.shape[0]
    send[:, :width] = mul(c_mate[...], w_out[...], NT).astype(BF16)
    send[:, width:] = nn(a_mate[...], w_out[...]).astype(BF16)


def own_body(a_own, c_own, w_ref, d_own, branch):
    d_own[...] = mul(c_own[...], w_ref[...], NT).astype(BF16)
    branch[...] = nn(a_own[...], w_ref[...])


def local(queries, key_rows, value_rows, out_proj, scale_ids, residual_in, cotangent):
    images, length, inner = queries.shape[1:]
    res = residual_in.shape[2]
    n = lax.axis_size("ba")
    sections = lax.axis_size("aa")
    block = out_proj.shape[1]
    tiles = inner // (2 * LANES)
    bits = (LANES // block).bit_length() - 1
    assert images == 1 and block << bits == LANES and bits > 0 and n == tiles << (bits + 1)
    weight = 1.0 / (n * images)

    def swap(value, by):
        return lax.ppermute(value, "ba", [(i, i ^ by) for i in range(n)])

    index = lax.axis_index("ba")
    own = (index >> bits) & 1
    upper = (index >> (bits - 1)) & 1
    top = index >> (bits + 1)
    place = jnp.stack([own, upper, top]).astype(jnp.int32)
    mate = 1 << bits
    side = 1 << (bits - 1)
    half = tiles // 2

    q, k, v = queries[0, 0], key_rows[0, 0], value_rows[0, 0]
    c_own = cotangent[0]

    blocks = [out_proj[0]] + [swap(out_proj[0], d << (bits + 1)) for d in range(1, tiles)]

    def gathered(parts):
        rows = jnp.stack(parts)
        for bit in range(bits - 1):
            other = swap(rows, 1 << bit)
            odd = ((index >> bit) & 1) == 1
            rows = jnp.concatenate([jnp.where(odd, other, rows), jnp.where(odd, rows, other)], axis=1)
        return rows, swap(rows, side)

    near, near_x = gathered(blocks[:half])
    c_mate = swap(c_own, mate)

    attn_shapes = (
        jax.ShapeDtypeStruct((2, length, inner // 2), BF16),
        jax.ShapeDtypeStruct((inner // HD, length, length), BF16),
    )
    attended, probs = call(forward_body, attn_shapes, 4 * length * length * inner * 4, "attend", n_vmem=5)(
        place, scale_ids.reshape(1, length), scale_ids.reshape(length, 1), q, k, v
    )
    a_own = attended[0]
    a_mate = swap(attended[1], mate)
    far, far_x = gathered(blocks[half:])

    def product(first):
        shapes = (
            jax.ShapeDtypeStruct((half, HD, res), F32),
            jax.ShapeDtypeStruct((half, HD, res), BF16),
        )
        body = functools.partial(product_body, first, weight)
        keep, send = call(body, shapes, 4 * length * half * LANES * res, f"product{first}", n_vmem=4)(
            place, a_own, a_mate, c_own, c_mate
        )
        total = keep + swap(send, side).astype(F32)
        for bit in reversed(range(bits - 1)):
            odd = ((index >> bit) & 1) == 1
            low, high = jnp.split(total, 2, axis=1)
            sent = jnp.where(odd, low, high).astype(BF16)
            total = jnp.where(odd, high, low) + swap(sent, 1 << bit).astype(F32)
        return total

    far_sum = product(half)
    near_sum = product(0)
    grad_proj = near_sum[0]
    for d in range(1, tiles):
        part = near_sum[d] if d < half else far_sum[d - half]
        grad_proj = grad_proj + swap(part.astype(BF16), d << (bits + 1)).astype(F32)

    width = inner // 2
    send, w_half = call(
        weights_body,
        (jax.ShapeDtypeStruct((length, width + res), BF16), jax.ShapeDtypeStruct((width, res), BF16)),
        4 * length * width * res,
        "partner",
        n_vmem=6,
    )(place, near, near_x, far, far_x, a_mate, c_mate)
    got = swap(send, mate)
    d_own, branch_own = call(
        own_body,
        (jax.ShapeDtypeStruct((length, width), BF16), jax.ShapeDtypeStruct((length, res), F32)),
        4 * length * width * res,
        "own",
        n_smem=0,
        n_vmem=3,
    )(a_own, c_own, w_half)

    branch = branch_own + got[:, width:].astype(F32)
    carried = branch
    pairs = [(i, i + 1) for i in range(sections - 1)]
    for _ in range(sections - 1):
        carried = branch + lax.ppermute(carried.astype(BF16), "aa", pairs).astype(F32)
    residual_out = (residual_in[0].astype(F32) + carried).astype(BF16)

    grad_shapes = (jax.ShapeDtypeStruct((length, inner), BF16),) * 3
    grads = ()
    for shift, d_rows in ((0, d_own), (1, got[:, :width])):
        body = functools.partial(backward_body, shift)
        given = (place, q, k, v, d_rows, probs)
        grads = pl.pallas_call(
            body,
            out_shape=grad_shapes,
            in_specs=[SMEM] + [VMEM] * (5 + len(grads)),
            out_specs=(VMEM,) * 3,
            compiler_params=PARAMS,
            cost_estimate=pl.CostEstimate(
                flops=16 * length * length * inner, bytes_accessed=1 << 20, transcendentals=0
            ),
            name=f"backward{shift}",
        )(*given, *grads)
    grad_q, grad_k, grad_v = grads
    return (
        residual_out[None, None],
        grad_q[None, None],
        grad_k[None, None],
        grad_v[None, None],
        grad_proj[None],
    )


def solution(mesh):
    placed = (
        P("aa", "ba", None, None),
        P("aa", "ba", None, None),
        P("aa", "ba", None, None),
        P("aa", "ba", None),
        P("ba", None),
        P("ba", None, None),
        P("ba", None, None),
    )
    return jax.shard_map(
        local,
        mesh=mesh,
        in_specs=placed,
        out_specs=(
            P("aa", "ba", None, None),
            P("aa", "ba", None, None),
            P("aa", "ba", None, None),
            P("aa", "ba", None, None),
            P("aa", "ba", None),
        ),
        check_vma=False,
    )
```

```python
import functools

import jax
import jax.numpy as jnp
from jax import lax
from jax.experimental import pallas as pl
from jax.experimental.pallas import tpu as pltpu
from jax.sharding import PartitionSpec as P


HD = 64
LANES = 128


VMEM = pl.BlockSpec(memory_space=pltpu.VMEM)
HBM = pl.BlockSpec(memory_space=pltpu.HBM)
NT = (((1,), (1,)), ((), ()))
TN = (((0,), (0,)), ((), ()))
LIMIT = 54656 << 10
F32 = jnp.float32
BF16 = jnp.bfloat16


def mul(a, b, dims):
    return lax.dot_general(a, b, dims, preferred_element_type=F32)


def nn(a, b):
    return jnp.dot(a, b, preferred_element_type=F32)


def tile(index):
    return pl.ds(pl.multiple_of(index * LANES, LANES), LANES)


def place_of(bits):
    index = lax.axis_index("ba")
    return (index >> bits) & 1, (index >> (bits - 1)) & 1, index >> (bits + 1)


def first_head(shape):
    return lax.broadcasted_iota(jnp.int32, shape, 1) < HD


def forward_body(bits, ids_hbm, q_hbm, k_hbm, v_hbm, mine, others, probs_hbm, ids_ref, q_ref, k_ref, v_ref, probs, arrived, left_for):
    own, _, _ = place_of(bits)
    length, inner = q_ref.shape
    pairs = inner // LANES
    bounds = (0, pairs // 8, pairs // 2, pairs)
    ids_copy = pltpu.make_async_copy(ids_hbm, ids_ref, arrived.at[3, 0])
    ids_copy.start()

    def copies(part):
        cols = pl.ds(bounds[part] * LANES, (bounds[part + 1] - bounds[part]) * LANES)
        return [
            pltpu.make_async_copy(source.at[:, cols], target.at[:, cols], arrived.at[kind, part])
            for kind, (source, target) in enumerate(((q_hbm, q_ref), (k_hbm, k_ref), (v_hbm, v_ref)))
        ]

    for part in range(3):
        for copy in copies(part):
            copy.start()
    ids_copy.wait()
    ids = jnp.broadcast_to(ids_ref[...].astype(F32), (8, length))
    visible = jnp.transpose(ids)[:, :1] <= ids[:1]
    left = first_head((length, LANES))
    stores = []
    even = None
    for part in range(3):
        for copy in copies(part):
            copy.wait()
        for pair in range(bounds[part], bounds[part + 1]):
            cols = pl.ds(pair * LANES, LANES)
            q_pair = q_ref[:, cols] * (HD**-0.5)
            k_pair = k_ref[:, cols]
            v_pair = v_ref[:, cols]
            halves = []
            for half in range(2):
                k_head = jnp.where(left == (half == 0), k_pair, jnp.zeros_like(k_pair))
                scores = jnp.where(visible, mul(k_head, q_pair, NT), -jnp.inf)
                lifted = jnp.exp(scores - jnp.max(scores, axis=0, keepdims=True))
                low = (lifted * (1.0 / jnp.sum(lifted, axis=0, keepdims=True))).astype(BF16)
                probs[2 * pair + half] = low
                halves.append(mul(low, v_pair, TN))
            heads = pl.ds(2 * pair, 2)
            stores.append(pltpu.make_async_copy(probs.at[heads], probs_hbm.at[heads], left_for.at[pair]))
            stores[-1].start()
            rows = jnp.where(left, halves[0], halves[1]).astype(BF16)
            if pair % 2 == 0:
                even = rows
            else:
                cols = pl.ds((pair // 2) * LANES, LANES)
                mine[:, cols] = jnp.where(own == 0, even, rows)
                others[:, cols] = jnp.where(own == 0, rows, even)
    for store in stores:
        store.wait()


def backward_pair(pair, refs, low_pair, d_pair, grads, block):
    q_ref, k_ref, v_ref = refs
    cols = tile(pair)
    left = first_head(d_pair.shape)
    q_pair = q_ref[:, cols] * (HD**-0.5)
    k_pair = k_ref[:, cols] * (HD**-0.5)
    v_pair = v_ref[:, cols]
    got = []
    for half, low in enumerate(low_pair):
        wide = low.astype(F32)
        v_head = jnp.where(left == (half == 0), v_pair, jnp.zeros_like(v_pair))
        d_probs = mul(v_head, d_pair, NT)
        delta = jnp.sum(wide * d_probs, axis=0, keepdims=True)
        d_scores = (wide * (d_probs - delta)).astype(BF16)
        got.append((mul(d_scores, k_pair, TN), nn(d_scores, q_pair), nn(low, d_pair)))
    for index, (one, two) in enumerate(zip(*got)):
        grads[index, :, block] = jnp.where(left, one, two).astype(BF16)


def backward_body(bits, shift, q_ref, k_ref, v_ref, probs, d_ref, *rest):
    outs, (grads, sems) = rest[-5:-2], rest[-2:]
    kind = place_of(bits)[0] ^ shift
    stores = []
    for step in range(sems.shape[1]):
        pair = 2 * step + kind
        block = pl.ds(step * LANES, LANES)
        if shift == 0:
            d_pair = mul(d_ref[...], rest[0][block, :], NT).astype(BF16)
        else:
            d_pair = d_ref[:, block]
        backward_pair(pair, (q_ref, k_ref, v_ref), (probs[2 * pair], probs[2 * pair + 1]), d_pair, grads, block)
        for index, out in enumerate(outs):
            stores.append(pltpu.make_async_copy(grads.at[index, :, block], out.at[:, tile(pair)], sems.at[index, step]))
            stores[-1].start()
    for store in stores:
        store.wait()


def product_body(bits, distances, weight, a_own, a_mate, c_own, c_mate, keep, send):
    _, upper, top = place_of(bits)
    for step, distance in enumerate(distances):
        cols = tile(jnp.bitwise_xor(top, distance))
        rows = mul(a_own[:, cols], c_own[...], TN) + mul(a_mate[:, cols], c_mate[...], TN)
        rows = rows * weight
        low, high = rows[:HD], rows[HD:]
        keep[step] = jnp.where(upper == 0, low, high)
        send[step] = jnp.where(upper == 0, high, low).astype(BF16)


def weights_body(bits, near, near_x, far, far_x, a_own, a_mate, c_mate, d_mate, branches, w_out):
    _, upper, top = place_of(bits)
    half = near.shape[0]
    for distance in range(2 * half):
        mine, other = (far, far_x) if distance % 2 else (near, near_x)
        base = jnp.bitwise_xor(top, distance) * LANES
        step = distance // 2
        w_out[pl.ds(pl.multiple_of(base + upper * HD, HD), HD), :] = mine[step]
        w_out[pl.ds(pl.multiple_of(base + (1 - upper) * HD, HD), HD), :] = other[step]
    res = w_out.shape[1]
    d_mate[...] = mul(c_mate[...], w_out[...], NT).astype(BF16)
    branches[:, :res] = nn(a_own[...], w_out[...]).astype(BF16)
    branches[:, res:] = nn(a_mate[...], w_out[...]).astype(BF16)


def step(queries, key_rows, value_rows, out_proj, scale_ids, residual_in, cotangent):
    images, length, inner = queries.shape[1:]
    res = residual_in.shape[2]
    n = lax.axis_size("ba")
    sections = lax.axis_size("aa")
    block = out_proj.shape[1]
    tiles = inner // (2 * LANES)
    bits = (LANES // block).bit_length() - 1
    assert images == 1 and block << bits == LANES and bits > 0 and n == tiles << (bits + 1) and tiles & (tiles - 1) == 0
    weight = 1.0 / (n * images)

    def swap(value, by):
        return lax.ppermute(value, "ba", [(i, i ^ by) for i in range(n)])

    def kernel(body, outs, flops, *given, hbm=0, out_specs=None, aliases={}, scratch=(), limit=24 << 20):
        return pl.pallas_call(
            body,
            out_shape=outs,
            in_specs=[VMEM] * (len(given) - hbm) + [HBM] * hbm,
            out_specs=out_specs or jax.tree.map(lambda _: VMEM, outs),
            input_output_aliases=aliases,
            scratch_shapes=scratch,
            compiler_params=pltpu.CompilerParams(vmem_limit_bytes=limit),
            cost_estimate=pl.CostEstimate(flops=flops, bytes_accessed=1 << 20, transcendentals=0),
        )(*given)

    def shaped(dtype, *dims):
        return jax.ShapeDtypeStruct(dims, dtype)

    index = lax.axis_index("ba")
    mate = 1 << bits
    side = 1 << (bits - 1)
    half = tiles // 2
    levels = tiles.bit_length() - 1
    width = inner // 2

    q, k, v = queries[0, 0], key_rows[0, 0], value_rows[0, 0]
    c_own = cotangent[0]

    c_mate = swap(c_own, mate)
    pairs = [(i, i + 1) for i in range(sections - 1)]
    near = out_proj
    for bit in reversed(range(1, levels)):
        near = jnp.stack([near, swap(near, mate << (bit + 1))], axis=1)
        near = near.reshape(-1, *out_proj.shape[1:])
    for bit in range(bits - 1):
        other = swap(near, 1 << bit)
        odd = ((index >> bit) & 1) == 1
        near = jnp.concatenate([jnp.where(odd, other, near), jnp.where(odd, near, other)], axis=1)
    far = swap(near, mate << 1)
    near_x = swap(near, side)

    far_x = swap(near_x, mate << 1)

    a_own, a_sent, probs = kernel(
        functools.partial(forward_body, bits),
        (shaped(BF16, length, width), shaped(BF16, length, width), shaped(BF16, inner // HD, length, length)),
        16 * length * length * inner,
        scale_ids, q, k, v,
        hbm=4,
        out_specs=(VMEM, VMEM, HBM),
        limit=LIMIT,
        scratch=[pltpu.VMEM((1, length), jnp.int32)]
        + [pltpu.VMEM((length, inner), BF16)] * 3
        + [pltpu.VMEM((inner // HD, length, length), BF16)]
        + [pltpu.SemaphoreType.DMA((4, 3)), pltpu.SemaphoreType.DMA((inner // LANES,))],
    )
    a_mate = swap(a_sent, mate)

    def product(distances):
        keep, send = kernel(
            functools.partial(product_body, bits, distances, weight),
            (shaped(F32, half, HD, res), shaped(BF16, half, HD, res)),
            4 * length * half * LANES * res,
            a_own, a_mate, c_own, c_mate,
        )
        total = keep + swap(send, side).astype(F32)
        for bit in reversed(range(bits - 1)):
            odd = ((index >> bit) & 1) == 1
            low, high = jnp.split(total, 2, axis=1)
            sent = jnp.where(odd, low, high).astype(BF16)
            total = jnp.where(odd, high, low) + swap(sent, 1 << bit).astype(F32)
        return total

    far_sum = product(range(1, tiles, 2))
    near_sum = product(range(0, tiles, 2))
    sums = near_sum + swap(far_sum.astype(BF16), mate << 1).astype(F32)
    for bit in range(1, levels):
        kept, sent = sums[0::2], sums[1::2]
        sums = kept + swap(sent.astype(BF16), mate << (bit + 1)).astype(F32)
    grad_proj = sums[0]

    d_mate, branches, w_half = kernel(
        functools.partial(weights_body, bits),
        (shaped(BF16, length, width), shaped(BF16, length, 2 * res), shaped(BF16, width, res)),
        6 * length * width * res,
        near, near_x, far, far_x, a_own, a_mate, c_mate,
    )
    d_got = swap(d_mate, mate)
    carried = branches
    for _ in range(sections - 1):
        passed = lax.ppermute(carried, "aa", pairs)
        carried = (branches.astype(F32) + passed.astype(F32)).astype(BF16)
    other = swap(carried[:, res:], mate)
    total = residual_in[0].astype(F32) + carried[:, :res].astype(F32) + other.astype(F32)
    residual_out = total.astype(BF16)

    grads = ()
    for shift, d_rows, rows in ((0, c_own, (w_half,)), (1, d_got, ())):
        grads = kernel(
            functools.partial(backward_body, bits, shift),
            (shaped(BF16, length, inner),) * 3,
            16 * length * length * inner,
            q, k, v, probs, d_rows, *rows, *grads,
            hbm=len(grads),
            out_specs=(HBM,) * 3,
            aliases={5 + i: i for i in range(len(grads))},
            scratch=[pltpu.VMEM((3, length, width), BF16), pltpu.SemaphoreType.DMA((3, tiles))],
        )
    grad_q, grad_k, grad_v = grads
    return (
        residual_out[None, None],
        grad_q[None, None],
        grad_k[None, None],
        grad_v[None, None],
        grad_proj[None],
    )


def solution(mesh):
    placed = (
        P("aa", "ba", None, None),
        P("aa", "ba", None, None),
        P("aa", "ba", None, None),
        P("aa", "ba", None),
        P("ba", None),
        P("ba", None, None),
        P("ba", None, None),
    )
    return jax.shard_map(
        step,
        mesh=mesh,
        in_specs=placed,
        out_specs=(
            P("aa", "ba", None, None),
            P("aa", "ba", None, None),
            P("aa", "ba", None, None),
            P("aa", "ba", None, None),
            P("aa", "ba", None),
        ),
        check_vma=False,
    )
```

```python
import functools

import jax
import jax.numpy as jnp
from jax import lax
from jax.experimental import pallas as pl
from jax.experimental.pallas import tpu as pltpu
from jax.sharding import PartitionSpec as P


HD = 64
LANES = 128


VMEM = pl.BlockSpec(memory_space=pltpu.VMEM)
HBM = pl.BlockSpec(memory_space=pltpu.HBM)
NT = (((1,), (1,)), ((), ()))
TN = (((0,), (0,)), ((), ()))
IDS_FLOPS = 1 << 32
F32 = jnp.float32
BF16 = jnp.bfloat16


def mul(a, b, dims):
    return lax.dot_general(a, b, dims, preferred_element_type=F32)


def nn(a, b):
    return jnp.dot(a, b, preferred_element_type=F32)


def tile(index):
    return pl.ds(pl.multiple_of(index * LANES, LANES), LANES)


def place_of(bits):
    index = lax.axis_index("ba")
    return (index >> bits) & 1, (index >> (bits - 1)) & 1, index >> (bits + 1)


def in_rows(parts):
    count, share = len(parts), parts[0].shape[0]
    section = lax.axis_index("aa")
    for hop, part in enumerate(parts):
        start = lax.rem(section + count - hop, count) * share
        yield pl.ds(pl.multiple_of(start, share), share), part


def first_head(shape):
    return lax.broadcasted_iota(jnp.int32, shape, 1) < HD


def ids_body(ids, out):
    out[...] = jnp.broadcast_to(ids[...].astype(F32), out.shape)


def forward_body(bits, ids_ref, q_ref, k_ref, v_ref, mine, others, probs):
    own, _, _ = place_of(bits)
    length, inner = q_ref.shape
    pairs = inner // LANES
    ids = ids_ref[...]
    visible = jnp.transpose(ids)[:, :1] <= ids[:1]
    left = first_head((length, LANES))

    def ahead(pair):
        cols = pl.ds(pair * LANES, LANES)
        q_pair = q_ref[:, cols] * (HD**-0.5)
        k_pair = k_ref[:, cols]
        return [mul(jnp.where(left == (half == 0), k_pair, jnp.zeros_like(k_pair)), q_pair, NT) for half in range(2)]

    following = ahead(0)
    for pair in range(pairs):
        scores = following
        if pair + 1 < pairs:
            following = ahead(pair + 1)
        v_pair = v_ref[:, pl.ds(pair * LANES, LANES)]
        halves = []
        for half in range(2):
            seen = jnp.where(visible, scores[half], -jnp.inf)
            lifted = jnp.exp(seen - jnp.max(seen, axis=0, keepdims=True))
            low = (lifted * (1.0 / jnp.sum(lifted, axis=0, keepdims=True))).astype(BF16)
            probs[2 * pair + half] = low
            halves.append(mul(low, v_pair, TN))
        rows = jnp.where(left, halves[0], halves[1]).astype(BF16)
        if pair % 2 == 0:
            even = rows
        else:
            cols = pl.ds((pair // 2) * LANES, LANES)
            mine[:, cols] = jnp.where(own == 0, even, rows)
            others[:, cols] = jnp.where(own == 0, rows, even)


def backward_pairs(refs, probs, jobs, grads, done):
    q_ref, k_ref, v_ref = refs

    def ahead(job):
        pair, d_pair, _ = job
        v_pair = v_ref[:, tile(pair)]
        left = first_head(v_pair.shape)
        return [mul(jnp.where(left == (half == 0), v_pair, jnp.zeros_like(v_pair)), d_pair, NT) for half in range(2)]

    following = ahead(jobs[0])
    for number, (pair, d_pair, block) in enumerate(jobs):
        d_probs = following
        if number + 1 < len(jobs):
            following = ahead(jobs[number + 1])
        cols = tile(pair)
        q_pair = q_ref[:, cols] * (HD**-0.5)
        k_pair = k_ref[:, cols] * (HD**-0.5)
        left = first_head(q_pair.shape)
        got = []
        for half in range(2):
            low = probs[2 * pair + half]
            wide = low.astype(F32)
            delta = jnp.sum(wide * d_probs[half], axis=0, keepdims=True)
            d_scores = (wide * (d_probs[half] - delta)).astype(BF16)
            got.append((mul(d_scores, k_pair, TN), nn(d_scores, q_pair), nn(low, d_pair)))
        for index, (one, two) in enumerate(zip(*got)):
            grads[index, :, block] = jnp.where(left, one, two).astype(BF16)
        done(block, pair)


def backward_own_body(bits, first, q_ref, k_ref, v_ref, probs, c_own, rows, rows_x, *rest):
    own, upper, top = place_of(bits)
    grads = rest[-1] if first else rest[-2]
    jobs = []
    for step in range(rows.shape[0]):
        pair = 2 * (top ^ (2 * step + first)) + own
        block = pl.ds(step * LANES, LANES)
        low = jnp.where(upper == 0, rows[step], rows_x[step])
        high = jnp.where(upper == 0, rows_x[step], rows[step])
        both = jnp.concatenate([low, high], axis=0)
        if first == 0:
            for held, part in in_rows(rest[:-2]):
                rest[-1][held, block] = mul(part[...], both, NT).astype(BF16)
        jobs.append((pair, mul(c_own[...], both, NT).astype(BF16), block))
    backward_pairs((q_ref, k_ref, v_ref), probs, jobs, grads, lambda *_: None)


def backward_mate_body(bits, q_ref, k_ref, v_ref, probs, d_near, d_far, near, far, *rest):
    outs, (grads, sems) = rest[:3], rest[3:]
    own, _, top = place_of(bits)
    tiles = sems.shape[1] // 2
    stores = []

    def store(source, block, pair, slot):
        for index, out in enumerate(outs):
            stores.append(pltpu.make_async_copy(source.at[index, :, block], out.at[:, tile(pair)], sems.at[index, slot]))
            stores[-1].start()

    for distance in range(tiles):
        block = pl.ds(distance // 2 * LANES, LANES)
        store(far if distance % 2 else near, block, 2 * (top ^ distance) + own, distance)
    jobs = []
    for distance in (*range(0, tiles, 2), *range(1, tiles, 2)):
        d_pair = (d_far if distance % 2 else d_near)[:, pl.ds(distance // 2 * LANES, LANES)]
        jobs.append((2 * (top ^ distance) + 1 - own, d_pair, pl.ds(distance * LANES, LANES)))

    def done(block, pair):
        store(grads, block, pair, len(stores) // 3)

    backward_pairs((q_ref, k_ref, v_ref), probs, jobs, grads, done)
    for copy in stores:
        copy.wait()


def finish_body(residual, branches, other, kept, arrived, out, grad_out):
    branch = branches[:, : out.shape[1]].astype(F32)
    out[...] = (residual[...].astype(F32) + branch + other[...].astype(F32)).astype(BF16)
    grad_out[...] = kept[...] + arrived[...].astype(F32)


def product_body(bits, distances, weight, a_own, a_mate, c_own, *rest):
    keep, send = rest[-2:]
    _, upper, top = place_of(bits)
    for step, distance in enumerate(distances):
        cols = tile(jnp.bitwise_xor(top, distance))
        rows = mul(a_own[:, cols], c_own[...], TN)
        for held, part in in_rows(rest[:-2]):
            rows = rows + mul(a_mate[held, cols], part[...], TN)
        rows = rows * weight
        low, high = rows[:HD], rows[HD:]
        keep[step] = jnp.where(upper == 0, low, high)
        send[step] = jnp.where(upper == 0, high, low).astype(BF16)


def weights_body(bits, near, near_x, far, far_x, a_own, a_mate, *rest):
    d_mate, branches, w_out = rest[-3:]
    _, upper, top = place_of(bits)
    half = near.shape[0]
    for distance in range(2 * half):
        mine, other = (far, far_x) if distance % 2 else (near, near_x)
        base = jnp.bitwise_xor(top, distance) * LANES
        step = distance // 2
        w_out[pl.ds(pl.multiple_of(base + upper * HD, HD), HD), :] = mine[step]
        w_out[pl.ds(pl.multiple_of(base + (1 - upper) * HD, HD), HD), :] = other[step]
    res = w_out.shape[1]
    for step in range(half):
        rows = w_out[tile(top ^ (2 * step + 1)), :]
        for held, part in in_rows(rest[:-3]):
            d_mate[held, pl.ds(step * LANES, LANES)] = mul(part[...], rows, NT).astype(BF16)
    branches[:, :res] = nn(a_own[...], w_out[...]).astype(BF16)
    branches[:, res:] = nn(a_mate[...], w_out[...]).astype(BF16)


def step(queries, key_rows, value_rows, out_proj, scale_ids, residual_in, cotangent):
    images, length, inner = queries.shape[1:]
    res = residual_in.shape[2]
    n = lax.axis_size("ba")
    sections = lax.axis_size("aa")
    block = out_proj.shape[1]
    tiles = inner // (2 * LANES)
    bits = (LANES // block).bit_length() - 1
    assert images == 1 and length % sections == 0 and block << bits == LANES and bits > 0 and n == tiles << (bits + 1) and tiles & (tiles - 1) == 0
    weight = 1.0 / (n * images)

    def swap(value, by):
        return lax.ppermute(value, "ba", [(i, i ^ by) for i in range(n)])

    def kernel(body, outs, flops, *given, hbm=0, out_specs=None, aliases={}, scratch=(), limit=24 << 20):
        return pl.pallas_call(
            body,
            out_shape=outs,
            in_specs=[VMEM] * (len(given) - hbm) + [HBM] * hbm,
            out_specs=out_specs or jax.tree.map(lambda _: VMEM, outs),
            input_output_aliases=aliases,
            scratch_shapes=scratch,
            compiler_params=pltpu.CompilerParams(vmem_limit_bytes=limit),
            cost_estimate=pl.CostEstimate(flops=flops, bytes_accessed=1 << 20, transcendentals=0),
        )(*given)

    def shaped(dtype, *dims):
        return jax.ShapeDtypeStruct(dims, dtype)

    index = lax.axis_index("ba")
    mate = 1 << bits
    side = 1 << (bits - 1)
    half = tiles // 2
    levels = tiles.bit_length() - 1
    width = inner // 2

    q, k, v = queries[0, 0], key_rows[0, 0], value_rows[0, 0]
    c_own = cotangent[0]

    section = lax.axis_index("aa")
    share = length // sections
    part = swap(lax.dynamic_slice_in_dim(c_own, section * share, share), mate)
    parts = [part]
    for hop in range(1, sections):
        parts.append(lax.ppermute(part, "aa", [(i, (i + hop) % sections) for i in range(sections)]))
    pairs = [(i, i + 1) for i in range(sections - 1)]
    near = out_proj
    for bit in reversed(range(1, levels)):
        near = jnp.stack([near, swap(near, mate << (bit + 1))], axis=1)
        near = near.reshape(-1, *out_proj.shape[1:])
    for bit in range(bits - 1):
        other = swap(near, 1 << bit)
        odd = ((index >> bit) & 1) == 1
        near = jnp.concatenate([jnp.where(odd, other, near), jnp.where(odd, near, other)], axis=1)
    far = swap(near, mate << 1)
    near_x = swap(near, side)

    far_x = swap(near_x, mate << 1)

    ids = kernel(ids_body, shaped(F32, 8, length), IDS_FLOPS, scale_ids)
    a_own, a_sent, probs = kernel(
        functools.partial(forward_body, bits),
        (shaped(BF16, length, width), shaped(BF16, length, width), shaped(BF16, inner // HD, length, length)),
        16 * length * length * inner,
        ids, q, k, v,
    )
    a_mate = swap(a_sent, mate)

    def product(distances):
        keep, send = kernel(
            functools.partial(product_body, bits, distances, weight),
            (shaped(F32, half, HD, res), shaped(BF16, half, HD, res)),
            4 * length * half * LANES * res,
            a_own, a_mate, c_own, *parts,
        )
        total = keep + swap(send, side).astype(F32)
        for bit in reversed(range(bits - 1)):
            odd = ((index >> bit) & 1) == 1
            low, high = jnp.split(total, 2, axis=1)
            sent = jnp.where(odd, low, high).astype(BF16)
            total = jnp.where(odd, high, low) + swap(sent, 1 << bit).astype(F32)
        return total

    far_sum = product(range(1, tiles, 2))
    near_sum = product(range(0, tiles, 2))
    sums = near_sum + swap(far_sum.astype(BF16), mate << 1).astype(F32)
    for bit in range(1, levels):
        kept, sent = sums[0::2], sums[1::2]
        arrived = swap(sent.astype(BF16), mate << (bit + 1))
        sums = kept + arrived.astype(F32)

    grads_near, d_mate = kernel(
        functools.partial(backward_own_body, bits, 0),
        (shaped(BF16, 3, length, half * LANES), shaped(BF16, length, half * LANES)),
        8 * length * length * inner,
        q, k, v, probs, c_own, near, near_x, *parts,
    )
    d_near = swap(d_mate, mate)

    d_mate, branches = kernel(
        functools.partial(weights_body, bits),
        (shaped(BF16, length, half * LANES), shaped(BF16, length, 2 * res)),
        6 * length * width * res,
        near, near_x, far, far_x, a_own, a_mate, *parts,
        scratch=[pltpu.VMEM((width, res), BF16)],
    )
    d_far = swap(d_mate, mate)
    carried = branches
    for _ in range(sections - 1):
        passed = lax.ppermute(carried, "aa", pairs)
        carried = (branches.astype(F32) + passed.astype(F32)).astype(BF16)
    other = swap(carried[:, res:], mate)
    residual_out, grad_proj = kernel(
        finish_body,
        (shaped(BF16, length, res), shaped(F32, block, res)),
        1 << 20,
        residual_in[0], carried, other, kept[0], arrived[0],
    )

    grads_far = kernel(
        functools.partial(backward_own_body, bits, 1),
        shaped(BF16, 3, length, half * LANES),
        8 * length * length * inner,
        q, k, v, probs, c_own, far, far_x,
    )
    grad_q, grad_k, grad_v = kernel(
        functools.partial(backward_mate_body, bits),
        (shaped(BF16, length, inner),) * 3,
        16 * length * length * inner,
        q, k, v, probs, d_near, d_far, grads_near, grads_far,
        out_specs=(HBM,) * 3,
        scratch=[pltpu.VMEM((3, length, width), BF16), pltpu.SemaphoreType.DMA((3, 2 * tiles))],
    )
    return (
        residual_out[None, None],
        grad_q[None, None],
        grad_k[None, None],
        grad_v[None, None],
        grad_proj[None],
    )


def solution(mesh):
    placed = (
        P("aa", "ba", None, None),
        P("aa", "ba", None, None),
        P("aa", "ba", None, None),
        P("aa", "ba", None),
        P("ba", None),
        P("ba", None, None),
        P("ba", None, None),
    )
    return jax.shard_map(
        step,
        mesh=mesh,
        in_specs=placed,
        out_specs=(
            P("aa", "ba", None, None),
            P("aa", "ba", None, None),
            P("aa", "ba", None, None),
            P("aa", "ba", None, None),
            P("aa", "ba", None),
        ),
        check_vma=False,
    )
```

```python
import functools

import jax
import jax.numpy as jnp
from jax import lax
from jax.experimental import pallas as pl
from jax.experimental.pallas import tpu as pltpu
from jax.sharding import PartitionSpec as P


HD = 64
LANES = 128


VMEM = pl.BlockSpec(memory_space=pltpu.VMEM)
HBM = pl.BlockSpec(memory_space=pltpu.HBM)
NT = (((1,), (1,)), ((), ()))
TN = (((0,), (0,)), ((), ()))
FIRST_FLOPS = 1 << 32
F32 = jnp.float32
BF16 = jnp.bfloat16


def mul(a, b, dims):
    return lax.dot_general(a, b, dims, preferred_element_type=F32)


def nn(a, b):
    return jnp.dot(a, b, preferred_element_type=F32)


def tile(index):
    return pl.ds(pl.multiple_of(index * LANES, LANES), LANES)


def place_of(bits):
    index = lax.axis_index("ba")
    return (index >> bits) & 1, (index >> (bits - 1)) & 1, index >> (bits + 1)


def in_rows(parts):
    count, share = len(parts), parts[0].shape[0]
    section = lax.axis_index("aa")
    for hop, part in enumerate(parts):
        start = lax.rem(section + count - hop, count) * share
        yield pl.ds(pl.multiple_of(start, share), share), part


def first_head(shape):
    return lax.broadcasted_iota(jnp.int32, shape, 1) < HD


def first_body(out):
    out[...] = first_head(out.shape).astype(F32)


def forward_body(bits, lanes, ids_ref, q_ref, k_ref, v_ref, mine, others, probs):
    own, _, _ = place_of(bits)
    length, inner = q_ref.shape
    pairs = inner // LANES
    ids = jnp.broadcast_to(ids_ref[...].astype(F32), (lanes.shape[0], length))
    visible = jnp.transpose(ids)[:, :1] <= ids[:1]
    left = jnp.broadcast_to(lanes[:1], (length, LANES)) > 0.5

    def ahead(pair):
        cols = pl.ds(pair * LANES, LANES)
        q_pair = q_ref[:, cols] * (HD**-0.5)
        k_pair = k_ref[:, cols]
        return [mul(jnp.where(left == (half == 0), k_pair, jnp.zeros_like(k_pair)), q_pair, NT) for half in range(2)]

    following = ahead(0)
    for pair in range(pairs):
        scores = following
        if pair + 1 < pairs:
            following = ahead(pair + 1)
        v_pair = v_ref[:, pl.ds(pair * LANES, LANES)]
        halves = []
        for half in range(2):
            seen = jnp.where(visible, scores[half], -jnp.inf)
            lifted = jnp.exp(seen - jnp.max(seen, axis=0, keepdims=True))
            low = (lifted * (1.0 / jnp.sum(lifted, axis=0, keepdims=True))).astype(BF16)
            probs[2 * pair + half] = low
            halves.append(mul(low, v_pair, TN))
        rows = jnp.where(left, halves[0], halves[1]).astype(BF16)
        if pair % 2 == 0:
            even = rows
        else:
            cols = pl.ds((pair // 2) * LANES, LANES)
            mine[:, cols] = jnp.where(own == 0, even, rows)
            others[:, cols] = jnp.where(own == 0, rows, even)


def backward_pairs(refs, probs, jobs, grads, done):
    q_ref, k_ref, v_ref = refs

    def ahead(job):
        pair, d_pair, _ = job
        v_pair = v_ref[:, tile(pair)]
        left = first_head(v_pair.shape)
        return [mul(jnp.where(left == (half == 0), v_pair, jnp.zeros_like(v_pair)), d_pair, NT) for half in range(2)]

    following = ahead(jobs[0])
    for number, (pair, d_pair, block) in enumerate(jobs):
        d_probs = following
        if number + 1 < len(jobs):
            following = ahead(jobs[number + 1])
        cols = tile(pair)
        q_pair = q_ref[:, cols] * (HD**-0.5)
        k_pair = k_ref[:, cols] * (HD**-0.5)
        left = first_head(q_pair.shape)
        got = []
        for half in range(2):
            low = probs[2 * pair + half]
            wide = low.astype(F32)
            delta = jnp.sum(wide * d_probs[half], axis=0, keepdims=True)
            d_scores = (wide * (d_probs[half] - delta)).astype(BF16)
            got.append((mul(d_scores, k_pair, TN), nn(d_scores, q_pair), nn(low, d_pair)))
        for index, (one, two) in enumerate(zip(*got)):
            grads[index, :, block] = jnp.where(left, one, two).astype(BF16)
        done(block, pair)


def backward_own_body(bits, first, q_ref, k_ref, v_ref, probs, c_own, rows, rows_x, *rest):
    own, upper, top = place_of(bits)
    grads = rest[-1] if first else rest[-2]
    jobs = []
    for step in range(rows.shape[0]):
        pair = 2 * (top ^ (2 * step + first)) + own
        block = pl.ds(step * LANES, LANES)
        low = jnp.where(upper == 0, rows[step], rows_x[step])
        high = jnp.where(upper == 0, rows_x[step], rows[step])
        both = jnp.concatenate([low, high], axis=0)
        if first == 0:
            for held, part in in_rows(rest[:-2]):
                rest[-1][held, block] = mul(part[...], both, NT).astype(BF16)
        jobs.append((pair, mul(c_own[...], both, NT).astype(BF16), block))
    backward_pairs((q_ref, k_ref, v_ref), probs, jobs, grads, lambda *_: None)


def backward_mate_body(bits, q_ref, k_ref, v_ref, probs, d_near, d_far, near, far, *rest):
    outs, (grads, sems) = rest[:3], rest[3:]
    own, _, top = place_of(bits)
    tiles = sems.shape[1] // 2
    stores = []

    def store(source, block, pair, slot):
        for index, out in enumerate(outs):
            stores.append(pltpu.make_async_copy(source.at[index, :, block], out.at[:, tile(pair)], sems.at[index, slot]))
            stores[-1].start()

    for distance in range(tiles):
        block = pl.ds(distance // 2 * LANES, LANES)
        store(far if distance % 2 else near, block, 2 * (top ^ distance) + own, distance)
    jobs = []
    for distance in (*range(0, tiles, 2), *range(1, tiles, 2)):
        d_pair = (d_far if distance % 2 else d_near)[:, pl.ds(distance // 2 * LANES, LANES)]
        jobs.append((2 * (top ^ distance) + 1 - own, d_pair, pl.ds(distance * LANES, LANES)))

    def done(block, pair):
        store(grads, block, pair, len(stores) // 3)

    backward_pairs((q_ref, k_ref, v_ref), probs, jobs, grads, done)
    for copy in stores:
        copy.wait()


def finish_body(residual, branches, other, kept, arrived, out, grad_out, total, grad_total, sems):
    length, res = total.shape
    grad_total[...] = kept[...] + arrived[...].astype(F32)
    copies = [pltpu.make_async_copy(grad_total, grad_out, sems.at[0])]
    copies[0].start()
    share = length // (sems.shape[0] - 1)
    for part in range(sems.shape[0] - 1):
        rows = pl.ds(part * share, share)
        branch = branches[rows, :res].astype(F32) + other[rows].astype(F32)
        total[rows] = (residual[rows].astype(F32) + branch).astype(BF16)
        copies.append(pltpu.make_async_copy(total.at[rows], out.at[rows], sems.at[part + 1]))
        copies[-1].start()
    for copy in copies:
        copy.wait()


def product_body(bits, distances, weight, a_own, a_mate, c_own, *rest):
    keep, send = rest[-2:]
    _, upper, top = place_of(bits)
    for step, distance in enumerate(distances):
        cols = tile(jnp.bitwise_xor(top, distance))
        rows = mul(a_own[:, cols], c_own[...], TN)
        for held, part in in_rows(rest[:-2]):
            rows = rows + mul(a_mate[held, cols], part[...], TN)
        rows = rows * weight
        low, high = rows[:HD], rows[HD:]
        keep[step] = jnp.where(upper == 0, low, high)
        send[step] = jnp.where(upper == 0, high, low).astype(BF16)


def weights_body(bits, near, near_x, far, far_x, a_own, a_mate, *rest):
    d_mate, branches, w_out = rest[-3:]
    _, upper, top = place_of(bits)
    half = near.shape[0]
    for distance in range(2 * half):
        mine, other = (far, far_x) if distance % 2 else (near, near_x)
        base = jnp.bitwise_xor(top, distance) * LANES
        step = distance // 2
        w_out[pl.ds(pl.multiple_of(base + upper * HD, HD), HD), :] = mine[step]
        w_out[pl.ds(pl.multiple_of(base + (1 - upper) * HD, HD), HD), :] = other[step]
    res = w_out.shape[1]
    for step in range(half):
        rows = w_out[tile(top ^ (2 * step + 1)), :]
        for held, part in in_rows(rest[:-3]):
            d_mate[held, pl.ds(step * LANES, LANES)] = mul(part[...], rows, NT).astype(BF16)
    branches[:, :res] = nn(a_own[...], w_out[...]).astype(BF16)
    branches[:, res:] = nn(a_mate[...], w_out[...]).astype(BF16)


def step(queries, key_rows, value_rows, out_proj, scale_ids, residual_in, cotangent):
    images, length, inner = queries.shape[1:]
    res = residual_in.shape[2]
    n = lax.axis_size("ba")
    sections = lax.axis_size("aa")
    block = out_proj.shape[1]
    tiles = inner // (2 * LANES)
    bits = (LANES // block).bit_length() - 1
    assert images == 1 and length % sections == 0 and block << bits == LANES and bits > 0 and n == tiles << (bits + 1) and tiles & (tiles - 1) == 0
    weight = 1.0 / (n * images)

    def swap(value, by):
        return lax.ppermute(value, "ba", [(i, i ^ by) for i in range(n)])

    def kernel(body, outs, flops, *given, hbm=0, out_specs=None, aliases={}, scratch=(), limit=24 << 20):
        return pl.pallas_call(
            body,
            out_shape=outs,
            in_specs=[VMEM] * (len(given) - hbm) + [HBM] * hbm,
            out_specs=out_specs or jax.tree.map(lambda _: VMEM, outs),
            input_output_aliases=aliases,
            scratch_shapes=scratch,
            compiler_params=pltpu.CompilerParams(vmem_limit_bytes=limit),
            cost_estimate=pl.CostEstimate(flops=flops, bytes_accessed=1 << 20, transcendentals=0),
        )(*given)

    def shaped(dtype, *dims):
        return jax.ShapeDtypeStruct(dims, dtype)

    index = lax.axis_index("ba")
    mate = 1 << bits
    side = 1 << (bits - 1)
    half = tiles // 2
    levels = tiles.bit_length() - 1
    width = inner // 2

    q, k, v = queries[0, 0], key_rows[0, 0], value_rows[0, 0]
    c_own = cotangent[0]

    section = lax.axis_index("aa")
    share = length // sections
    part = swap(lax.dynamic_slice_in_dim(c_own, section * share, share), mate)
    parts = [part]
    for hop in range(1, sections):
        parts.append(lax.ppermute(part, "aa", [(i, (i + hop) % sections) for i in range(sections)]))
    pairs = [(i, i + 1) for i in range(sections - 1)]
    near = out_proj
    for bit in reversed(range(1, levels)):
        near = jnp.stack([near, swap(near, mate << (bit + 1))], axis=1)
        near = near.reshape(-1, *out_proj.shape[1:])
    for bit in range(bits - 1):
        other = swap(near, 1 << bit)
        odd = ((index >> bit) & 1) == 1
        near = jnp.concatenate([jnp.where(odd, other, near), jnp.where(odd, near, other)], axis=1)
    far = swap(near, mate << 1)
    near_x = swap(near, side)

    far_x = swap(near_x, mate << 1)

    lanes = kernel(first_body, shaped(F32, 8, LANES), FIRST_FLOPS)
    a_own, a_sent, probs = kernel(
        functools.partial(forward_body, bits),
        (shaped(BF16, length, width), shaped(BF16, length, width), shaped(BF16, inner // HD, length, length)),
        16 * length * length * inner,
        lanes, scale_ids, q, k, v,
    )
    a_mate = swap(a_sent, mate)

    def product(distances):
        keep, send = kernel(
            functools.partial(product_body, bits, distances, weight),
            (shaped(F32, half, HD, res), shaped(BF16, half, HD, res)),
            4 * length * half * LANES * res,
            a_own, a_mate, c_own, *parts,
        )
        total = keep + swap(send, side).astype(F32)
        for bit in reversed(range(bits - 1)):
            odd = ((index >> bit) & 1) == 1
            low, high = jnp.split(total, 2, axis=1)
            sent = jnp.where(odd, low, high).astype(BF16)
            total = jnp.where(odd, high, low) + swap(sent, 1 << bit).astype(F32)
        return total

    far_sum = product(range(1, tiles, 2))
    near_sum = product(range(0, tiles, 2))
    sums = near_sum + swap(far_sum.astype(BF16), mate << 1).astype(F32)
    for bit in range(1, levels):
        kept, sent = sums[0::2], sums[1::2]
        arrived = swap(sent.astype(BF16), mate << (bit + 1))
        sums = kept + arrived.astype(F32)

    grads_near, d_mate = kernel(
        functools.partial(backward_own_body, bits, 0),
        (shaped(BF16, 3, length, half * LANES), shaped(BF16, length, half * LANES)),
        8 * length * length * inner,
        q, k, v, probs, c_own, near, near_x, *parts,
    )
    d_near = swap(d_mate, mate)

    d_mate, branches = kernel(
        functools.partial(weights_body, bits),
        (shaped(BF16, length, half * LANES), shaped(BF16, length, 2 * res)),
        6 * length * width * res,
        near, near_x, far, far_x, a_own, a_mate, *parts,
        scratch=[pltpu.VMEM((width, res), BF16)],
    )
    d_far = swap(d_mate, mate)
    carried = branches
    for _ in range(sections - 1):
        passed = lax.ppermute(carried, "aa", pairs)
        carried = (branches.astype(F32) + passed.astype(F32)).astype(BF16)
    other = swap(carried[:, res:], mate)
    residual_out, grad_proj = kernel(
        finish_body,
        (shaped(BF16, length, res), shaped(F32, block, res)),
        1 << 20,
        residual_in[0], carried, other, kept[0], arrived[0],
        out_specs=(HBM, HBM),
        scratch=[pltpu.VMEM((length, res), BF16), pltpu.VMEM((block, res), F32), pltpu.SemaphoreType.DMA((4,))],
    )

    grads_far = kernel(
        functools.partial(backward_own_body, bits, 1),
        shaped(BF16, 3, length, half * LANES),
        8 * length * length * inner,
        q, k, v, probs, c_own, far, far_x,
    )
    grad_q, grad_k, grad_v = kernel(
        functools.partial(backward_mate_body, bits),
        (shaped(BF16, length, inner),) * 3,
        16 * length * length * inner,
        q, k, v, probs, d_near, d_far, grads_near, grads_far,
        out_specs=(HBM,) * 3,
        scratch=[pltpu.VMEM((3, length, width), BF16), pltpu.SemaphoreType.DMA((3, 2 * tiles))],
    )
    return (
        residual_out[None, None],
        grad_q[None, None],
        grad_k[None, None],
        grad_v[None, None],
        grad_proj[None],
    )


def solution(mesh):
    placed = (
        P("aa", "ba", None, None),
        P("aa", "ba", None, None),
        P("aa", "ba", None, None),
        P("aa", "ba", None),
        P("ba", None),
        P("ba", None, None),
        P("ba", None, None),
    )
    return jax.shard_map(
        step,
        mesh=mesh,
        in_specs=placed,
        out_specs=(
            P("aa", "ba", None, None),
            P("aa", "ba", None, None),
            P("aa", "ba", None, None),
            P("aa", "ba", None, None),
            P("aa", "ba", None),
        ),
        check_vma=False,
    )
```
